128 devices in a mesh: branch: 2 (over core), dp: 8 (over x, z_hi), mp: 8 (over z_lo, y).
Axes of the slice: x: 4, y: 4, z: 4 (z_hi: 2, z_lo: 2; z = z_hi * 2 + z_lo), core: 2. Of those that a mesh axis runs over, the one named last changes fastest.
Arguments:
- unet_hidden: bfloat16 [16, 1280, 256], P(('branch', 'dp'), 'mp'), may hold values from -6 to 6
- control_hidden: bfloat16 [2, 2, 8, 1280, 256], P('branch', None, 'dp', 'mp'), may hold values from -6 to 6
- timesteps: int32 [2, 8], P(None, 'dp'), may hold values from 0 to 999
- control_scales: int32 [2, 2, 8], P('branch', None, 'dp'), may hold values from 1 to 16
- unet_time_first: bfloat16 [320, 1280], replicated, may hold values from -0.3125 to 0.3125
- unet_time_second: bfloat16 [1280, 1280], replicated, may hold values from -0.15625 to 0.15625
- unet_proj: bfloat16 [1280, 1280], P(None, 'mp'), may hold values from -0.15625 to 0.15625
- unet_conv_first: bfloat16 [9, 1280, 1280], P(None, 'mp'), may hold values from -0.0546875 to 0.0546875
- unet_conv_second: bfloat16 [9, 1280, 1280], P(None, 'mp'), may hold values from -0.0546875 to 0.0546875
- control_time_first: bfloat16 [2, 320, 1280], P('branch'), may hold values from -0.3125 to 0.3125
- control_time_second: bfloat16 [2, 1280, 1280], P('branch'), may hold values from -0.15625 to 0.15625
- control_proj: bfloat16 [2, 1280, 1280], P('branch', None, 'mp'), may hold values from -0.15625 to 0.15625
- control_conv_first: bfloat16 [2, 9, 1280, 1280], P('branch', None, 'mp'), may hold values from -0.0546875 to 0.0546875
- control_conv_second: bfloat16 [2, 9, 1280, 1280], P('branch', None, 'mp'), may hold values from -0.0546875 to 0.0546875
- zero_conv: bfloat16 [2, 1280, 1280], P('branch', 'mp'), may hold values from -0.15625 to 0.15625
Outputs:
- skip_out: bfloat16 [16, 1280, 256], P(('branch', 'dp'), 'mp')
The draws below stay inside these ranges and needn't reach their ends.
All inputs are finite; a program needn't handle non-finite values.
Results may differ from the reference program's by a relative error of at most 0.018.
Values may be sent and summed in bfloat16 or wider, within the bound.
A program may use at most 128 MiB of HBM per device.

```python
import math
import jax
import jax.numpy as jnp
from jax import lax

C = 1280
TDIM = 320
GROUPS = 32
SIDE = 16
COPIES = 2
HW = 256
HALVES = 2
BATCH = 16


def plant(entries, key, smallest, high):
    index_at = [jax.random.randint(jax.random.fold_in(key, axis), (), 0, length) for axis, length in enumerate(entries.shape)]
    main_axis = entries.shape.index(max(entries.shape))
    beside = index_at[:main_axis] + [(index_at[main_axis] + 1) % entries.shape[main_axis]] + index_at[main_axis + 1:]
    return entries.at[tuple(index_at)].set(smallest).at[tuple(beside)].set(high)


def shard_levels(rng, extent, split, smallest, top_value):
    factor_of, own = 1.0, jax.random.fold_in(rng, 6)
    for dim, parts in split:
        heights = jnp.exp(jax.random.uniform(jax.random.fold_in(own, dim), (parts,), jnp.float32, smallest / len(split), top_value / len(split)))
        factor_of = factor_of * jnp.repeat(heights, extent[dim] // parts).reshape([-1 if axis == dim else 1 for axis in range(len(extent))])
    return factor_of


def centred(stream_key, extent, deviation, most, cuts=(), held_as=jnp.bfloat16):
    level = shard_levels(stream_key, extent, cuts, -0.22, 0.18) if cuts else 1.0
    array = jax.random.normal(stream_key, extent, jnp.float32) * deviation * level
    return jnp.minimum(jnp.maximum(array, -most), most).astype(held_as)


def setup_inputs(seed: int = 0) -> dict:
    key_list = jax.random.split(jax.random.key(seed), 16)
    unet_hidden = centred(key_list[0], (BATCH, C, HW), 1.0, 6.0, ((0, 16), (1, 8)))
    control_hidden = centred(key_list[1], (COPIES, HALVES, BATCH // HALVES, C, HW), 1.0, 6.0, ((0, 2), (2, 8), (3, 8)))
    timesteps = plant(jax.random.randint(key_list[2], (HALVES, BATCH // HALVES), 0, 1000), jax.random.fold_in(key_list[2], 1), 0, 999).astype(jnp.int32)
    control_scales = plant(jax.random.randint(key_list[3], (COPIES, HALVES, BATCH // HALVES), 1, 17), jax.random.fold_in(key_list[3], 1), 1, 16).astype(jnp.int32)
    unet_time_first = centred(key_list[4], (TDIM, C), TDIM ** -0.5, 0.3125)
    unet_time_second = centred(key_list[5], (C, C), C ** -0.5, 0.15625)
    unet_proj = centred(key_list[6], (C, C), C ** -0.5, 0.15625, ((1, 8),))
    unet_conv_first = centred(key_list[7], (9, C, C), (9 * C) ** -0.5, 0.0546875, ((1, 8),))
    unet_conv_second = centred(key_list[8], (9, C, C), (9 * C) ** -0.5, 0.0546875, ((1, 8),))
    control_time_first = centred(key_list[9], (COPIES, TDIM, C), TDIM ** -0.5, 0.3125, ((0, 2),))
    control_time_second = centred(key_list[10], (COPIES, C, C), C ** -0.5, 0.15625, ((0, 2),))
    control_proj = centred(key_list[11], (COPIES, C, C), C ** -0.5, 0.15625, ((0, 2), (2, 8)))
    control_conv_first = centred(key_list[12], (COPIES, 9, C, C), (9 * C) ** -0.5, 0.0546875, ((0, 2), (2, 8)))
    control_conv_second = centred(key_list[13], (COPIES, 9, C, C), (9 * C) ** -0.5, 0.0546875, ((0, 2), (2, 8)))
    zero_conv = centred(key_list[14], (COPIES, C, C), C ** -0.5, 0.15625, ((0, 2), (1, 8)))
    return dict(unet_hidden=unet_hidden, control_hidden=control_hidden, timesteps=timesteps, control_scales=control_scales, unet_time_first=unet_time_first, unet_time_second=unet_time_second, unet_proj=unet_proj, unet_conv_first=unet_conv_first, unet_conv_second=unet_conv_second, control_time_first=control_time_first, control_time_second=control_time_second, control_proj=control_proj, control_conv_first=control_conv_first, control_conv_second=control_conv_second, zero_conv=zero_conv)


def sinusoid(step_ids):
    half_width = TDIM // 2
    frequency = jnp.exp(-math.log(10000.0) * jnp.arange(half_width, dtype=jnp.float32) / half_width)
    angles = step_ids.astype(jnp.float32)[:, None] * frequency[None, :]
    return jnp.concatenate([jnp.cos(angles), jnp.sin(angles)], axis=1)

def time_embed(step_ids, first_weight, second_weight):
    waves = sinusoid(step_ids).astype(jnp.bfloat16)
    middle = jax.nn.silu(jnp.dot(waves, first_weight, preferred_element_type=jnp.float32)).astype(jnp.bfloat16)
    embedded = jnp.dot(middle, second_weight, preferred_element_type=jnp.float32)
    return jax.nn.silu(embedded).astype(jnp.bfloat16)

def norm_silu(values):
    image_count, width, pixels = values.shape
    group_size = C // GROUPS
    grouped = values.reshape(image_count, width // group_size, group_size, pixels)
    group_mean = lax.optimization_barrier(jnp.mean(grouped, axis=(2, 3), keepdims=True))
    centered = grouped - group_mean
    group_var = lax.optimization_barrier(jnp.mean(centered * centered, axis=(2, 3), keepdims=True))
    normed = centered * lax.rsqrt(group_var + 1e-05)
    return jax.nn.silu(normed).reshape(image_count, width, pixels)

def conv_taps(activation, weight, einsum_form):
    image_count, width, pixels = activation.shape
    image_grid = activation.astype(jnp.float32).reshape(image_count, width, SIDE, SIDE)
    padded = jnp.pad(image_grid, ((0, 0), (0, 0), (1, 1), (1, 1)))
    accum_sum = None
    for tap_index in range(9):
        row_shift = tap_index // 3
        col_shift = tap_index % 3
        window = padded[:, :, row_shift:row_shift + SIDE, col_shift:col_shift + SIDE].reshape(image_count, width, pixels)
        term = jnp.einsum(einsum_form, weight[tap_index].astype(jnp.float32), window, precision=lax.Precision.HIGHEST)
        accum_sum = term if accum_sum is None else accum_sum + term
    return accum_sum

def resnet_block(hidden, conv_first, conv_second, time_proj, time_act):
    first_act = norm_silu(hidden.astype(jnp.float32)).astype(jnp.bfloat16)
    inner_sum = conv_taps(first_act, conv_first, 'oc,bcp->bop')
    inner_sum = inner_sum + jnp.dot(time_act, time_proj, preferred_element_type=jnp.float32)[:, :, None]
    second_act = norm_silu(inner_sum).astype(jnp.bfloat16)
    return hidden.astype(jnp.float32) + conv_taps(second_act, conv_second, 'co,bcp->bop')

def reference(unet_hidden, control_hidden, timesteps, control_scales, unet_time_first, unet_time_second, unet_proj, unet_conv_first, unet_conv_second, control_time_first, control_time_second, control_proj, control_conv_first, control_conv_second, zero_conv):
    step_ids = timesteps.reshape(BATCH)
    unet_act = time_embed(step_ids, unet_time_first, unet_time_second)
    unet_out = resnet_block(unet_hidden, unet_conv_first, unet_conv_second, unet_proj, unet_act)
    residual = jnp.zeros((BATCH, C, HW), jnp.float32)
    for copy_index in range(COPIES):
        copy_act = time_embed(step_ids, control_time_first[copy_index], control_time_second[copy_index])
        copy_hidden = control_hidden[copy_index].reshape(BATCH, C, HW)
        copy_out = resnet_block(copy_hidden, control_conv_first[copy_index], control_conv_second[copy_index], control_proj[copy_index], copy_act).astype(jnp.bfloat16)
        scale_factor = control_scales[copy_index].reshape(BATCH).astype(jnp.float32) / 8.0
        zero_terms = jnp.einsum('co,bcp->bop', zero_conv[copy_index].astype(jnp.float32), copy_out.astype(jnp.float32), precision=lax.Precision.HIGHEST)
        residual = residual + scale_factor[:, None, None] * zero_terms
    return (unet_out + residual).astype(jnp.bfloat16)
```

```python
import functools
import math

import jax
import jax.numpy as jnp
from jax import lax
from jax.experimental import pallas as pl
from jax.experimental.pallas import tpu as pltpu
from jax.sharding import PartitionSpec as P

C = 1280
TDIM = 320
SIDE = 16
PIX = 256
WIDTH = 160
GROUP = 40
HALF = 80
TAPS = 9
KPAD = 1536
ZPAD = 256
PARTS = 2
LANES = PIX // PARTS
MESH = pl.DeviceIdType.MESH
F32 = jnp.float32
BF16 = jnp.bfloat16


def silu(v):
    return v * 0.5 * (1.0 + jnp.tanh(v * 0.5))


def norm_silu(values):
    grouped = values.reshape(WIDTH // GROUP, GROUP, PIX)
    scale = 1.0 / (GROUP * PIX)
    mean = jnp.sum(jnp.sum(grouped, axis=1, keepdims=True), axis=2, keepdims=True) * scale
    centered = grouped - mean
    var = jnp.sum(jnp.sum(centered * centered, axis=1, keepdims=True), axis=2, keepdims=True) * scale
    return silu(centered * lax.rsqrt(var + 1e-05)).reshape(WIDTH, PIX)


def shifted(values, step, pixel):
    return pltpu.roll(values, (-step) % PIX, 1)


def kernel(
    ts_ref, sc_ref, uh, ch, utf, uts, upr, uc1, uc2, ctf, cts, cpr, cc1, cc2, zc,
    out_ref,
    hid, act, w1, w2, w2t, tf, tw, pr, zw, zt, tpt, inner, shifts, part, co, zs, zr,
    st1, st2, st3, r1, r2, r3,
    load_sem, ag_send, ag_recv, s1, s2, s3, v1, v2, v3, swap_send, swap_recv,
):
    branch = lax.axis_index("branch")
    spot = lax.axis_index("mp")
    z = spot // 4
    y = spot % 4
    zo = 1 - z
    yp, ym, y2 = (y + 1) % 4, (y + 3) % 4, (y + 2) % 4
    up = {"mp": z * 4 + yp}
    down = {"mp": z * 4 + ym}
    across = {"mp": zo * 4 + y}
    partner = {"branch": 1 - branch}
    columns = (y2, yp, ym, y)

    sent = []

    def send(src, dst, ssem, rsem, target):
        copy = pltpu.make_async_remote_copy(
            src_ref=src, dst_ref=dst, send_sem=ssem, recv_sem=rsem, device_id=target, device_id_type=MESH
        )
        copy.start()
        sent.append(copy)

    def arrived(dst, rsem, ssem):
        pltpu.make_async_remote_copy(
            src_ref=dst, dst_ref=dst, send_sem=ssem, recv_sem=rsem, device_id=up, device_id_type=MESH
        ).wait_recv()

    barrier = pltpu.get_barrier_semaphore()
    for target in (up, down, across, partner):
        pl.semaphore_signal(barrier, inc=1, device_id=target, device_id_type=MESH)

    loads = {}

    def load(name, src, dst):
        loads[name] = pltpu.make_async_copy(src, dst, load_sem.at[len(loads)])
        loads[name].start()

    load("h0", ch.at[1 - branch], hid.at[0])
    load("h1", ch.at[branch], hid.at[1])
    load("h2", uh, hid.at[2])
    load("ctf", ctf, tf.at[0])
    load("cts", cts, tw.at[0])
    load("cpr", cpr, pr.at[0])
    load("cc1", cc1, w1.at[0])
    load("cc2", cc2, w2.at[0, pl.ds(0, TAPS * WIDTH)])
    load("utf", utf, tf.at[1])
    load("uts", uts, tw.at[1])
    load("upr", upr, pr.at[1])
    load("zc", zc, zw.at[pl.ds(0, WIDTH)])
    load("uc1", uc1, w1.at[1])
    load("uc2", uc2, w2.at[1, pl.ds(0, TAPS * WIDTH)])

    def rows(zz, yy):
        return pl.multiple_of((zz * 4 + yy) * WIDTH, 32)

    def piece(i, zz, yy, start=0, size=WIDTH):
        return act.at[i, pl.ds(pl.multiple_of(rows(zz, yy) + start, 16), size)]

    def normed(i, name):
        loads[name].wait()
        act[i, pl.ds(rows(z, y), WIDTH), :] = norm_silu(hid[i].astype(F32)).astype(BF16)

    def ag_own(i):
        own = piece(i, z, y)
        send(own, own, ag_send.at[i, 0], ag_recv.at[i, 0], across)
        send(own, own, ag_send.at[i, 1], ag_recv.at[i, 1], up)
        send(own, own, ag_send.at[i, 2], ag_recv.at[i, 2], down)

    def ag_a(i):
        got = piece(i, zo, y)
        arrived(got, ag_recv.at[i, 0], ag_send.at[i, 0])
        send(got, got, ag_send.at[i, 3], ag_recv.at[i, 3], up)
        send(got, got, ag_send.at[i, 4], ag_recv.at[i, 4], down)

    def ag_relay(i, zz, first, second):
        arrived(piece(i, zz, ym), ag_recv.at[i, first], ag_send.at[i, first])
        low = piece(i, zz, ym, 0, HALF)
        send(low, low, ag_send.at[i, second], ag_recv.at[i, second], up)
        arrived(piece(i, zz, yp), ag_recv.at[i, first + 1], ag_send.at[i, first + 1])
        high = piece(i, zz, yp, HALF, HALF)
        send(high, high, ag_send.at[i, second + 1], ag_recv.at[i, second + 1], down)

    def ag_b(i):
        ag_relay(i, z, 1, 5)

    def ag_c(i):
        ag_relay(i, zo, 3, 7)

    def ag_done(i):
        for zz, first in ((z, 5), (zo, 7)):
            arrived(piece(i, zz, y2, 0, HALF), ag_recv.at[i, first], ag_send.at[i, first])
            arrived(piece(i, zz, y2, HALF, HALF), ag_recv.at[i, first + 1], ag_send.at[i, first + 1])

    pixel = lax.broadcasted_iota(jnp.int32, (1, PIX), 1)
    column = pixel % SIDE
    not_left, not_right = column >= 1, column <= SIDE - 2
    not_top, not_bottom = pixel >= SIDE, pixel < PIX - SIDE

    def waves():
        lane = lax.broadcasted_iota(jnp.int32, (16, TDIM), 1)
        row = lax.broadcasted_iota(jnp.int32, (16, TDIM), 0)
        half_width = TDIM // 2
        index = jnp.where(lane < half_width, lane, lane - half_width).astype(F32)
        frequency = jnp.exp(-math.log(10000.0) * index / half_width)
        step = jnp.where(row == 0, ts_ref[0, 0].astype(F32), ts_ref[1, 0].astype(F32))
        angle = step * frequency
        return jnp.where(lane < half_width, jnp.cos(angle), jnp.sin(angle)).astype(BF16)

    def embed(k, first, second, third):
        loads[first].wait()
        middle = silu(jnp.dot(waves(), tf[k], preferred_element_type=F32)).astype(BF16)
        loads[second].wait()
        time_act = silu(jnp.dot(middle, tw[k], preferred_element_type=F32)).astype(BF16)
        loads[third].wait()
        projected = jnp.dot(time_act, pr[k], preferred_element_type=F32)
        wide = jnp.concatenate([projected, jnp.zeros((16, ZPAD - WIDTH), F32)], axis=1)
        tall = jnp.concatenate([wide, jnp.zeros((128 - 16, ZPAD), F32)], axis=0)
        tpt[k] = tall.T

    def time_column(k, half):
        lane = lax.broadcasted_iota(jnp.int32, (WIDTH, 128), 1)
        return jnp.sum(jnp.where(lane == half, tpt[k, 0:WIDTH, :], 0.0), axis=1, keepdims=True)

    def turned(src, dst):
        def body(j, carry):
            at = pl.multiple_of(j * 128, 128)
            dst[pl.ds(at, 128), :] = src[:, pl.ds(at, 128)].T
            return carry

        lax.fori_loop(0, C // 128, body, 0)

    def conv_first(i, k, dy):
        product = jnp.dot(
            w1[k, dy * 3 * WIDTH : (dy + 1) * 3 * WIDTH, :], act[i], preferred_element_type=F32
        )
        left = jnp.where(not_left, shifted(product[0:WIDTH], -1, pixel), 0.0)
        right = jnp.where(not_right, shifted(product[2 * WIDTH : 3 * WIDTH], 1, pixel), 0.0)
        total = left + product[WIDTH : 2 * WIDTH] + right
        if dy == 0:
            inner[...] = jnp.where(not_top, shifted(total, -SIDE, pixel), 0.0)
        elif dy == 1:
            inner[...] += total
        else:
            inner[...] += jnp.where(not_bottom, shifted(total, SIDE, pixel), 0.0)

    def second_operand(k, half):
        second = norm_silu(inner[...] + time_column(k, half))
        left = jnp.where(not_left, shifted(second, -1, pixel), 0.0)
        right = jnp.where(not_right, shifted(second, 1, pixel), 0.0)
        for dx, value in enumerate((left, second, right)):
            top = jnp.where(not_top, shifted(value, -SIDE, pixel), 0.0)
            bottom = jnp.where(not_bottom, shifted(value, SIDE, pixel), 0.0)
            for dy, moved in enumerate((top, value, bottom)):
                at = (dy * 3 + dx) * WIDTH
                shifts[at : at + WIDTH, :] = moved.astype(BF16)

    def both_planes(ref, yy):
        return jnp.concatenate([ref[pl.ds(rows(0, yy), WIDTH), :], ref[pl.ds(rows(1, yy), WIDTH), :]], axis=0)

    def conv_second(i, k, c):
        product = jnp.dot(both_planes(w2t.at[k], columns[c]), shifts[...], preferred_element_type=F32)
        part[i, c] = product.reshape(2, WIDTH, PIX)

    def lanes(h):
        return slice(h * LANES, (h + 1) * LANES)

    def rs1(i, h):
        st1[i, h] = part[i, 0, :, :, lanes(h)].astype(BF16)
        send(st1.at[i, h, :, pl.ds(0, HALF)], r1.at[i, h, 0], s1.at[i, h, 0], v1.at[i, h, 0], up)
        send(st1.at[i, h, :, pl.ds(HALF, HALF)], r1.at[i, h, 1], s1.at[i, h, 1], v1.at[i, h, 1], down)

    def rs2(i, h):
        for side, target in ((0, up), (1, down)):
            arrived(r1.at[i, h, side], v1.at[i, h, side], s1.at[i, h, side])
            plus = slice(side * HALF, (side + 1) * HALF)
            other = slice((1 - side) * HALF, (2 - side) * HALF)
            st2[i, h, side, :, plus, :] = (
                part[i, 1 + side, :, plus, lanes(h)] + r1[i, h, side].astype(F32)
            ).astype(BF16)
            st2[i, h, side, :, other, :] = part[i, 1 + side, :, other, lanes(h)].astype(BF16)
            send(st2.at[i, h, side], r2.at[i, h, side], s2.at[i, h, side], v2.at[i, h, side], target)

    def column_sum(i, h, zz):
        return part[i, 3, zz, :, lanes(h)] + r2[i, h, 0, zz].astype(F32) + r2[i, h, 1, zz].astype(F32)

    def rs3(i, h):
        for side in range(2):
            arrived(r2.at[i, h, side], v2.at[i, h, side], s2.at[i, h, side])
        st3[i, h] = column_sum(i, h, zo).astype(BF16)
        send(st3.at[i, h], r3.at[i, h], s3.at[i, h], v3.at[i, h], across)

    def summed(i, h):
        arrived(r3.at[i, h], v3.at[i, h], s3.at[i, h])
        return hid[i, :, lanes(h)].astype(F32) + column_sum(i, h, z) + r3[i, h].astype(F32)

    def zero_terms(c, scale, h):
        product = jnp.dot(both_planes(zt, columns[c]), co[:, lanes(h)], preferred_element_type=F32)
        return (product * scale).reshape(2, WIDTH, LANES)

    normed(0, "h0")
    pl.semaphore_wait(barrier, 4)
    ag_own(0)
    normed(1, "h1")
    ag_own(1)
    normed(2, "h2")
    for k in range(2):
        w2[k, TAPS * WIDTH : KPAD, :] = jnp.zeros((KPAD - TAPS * WIDTH, C), BF16)
    shifts[TAPS * WIDTH : KPAD, :] = jnp.zeros((KPAD - TAPS * WIDTH, PIX), BF16)
    zw[WIDTH:ZPAD, :] = jnp.zeros((ZPAD - WIDTH, C), BF16)
    co[WIDTH:ZPAD, :] = jnp.zeros((ZPAD - WIDTH, PIX), BF16)
    ag_a(0)
    ag_b(0)
    ag_own(2)
    embed(0, "ctf", "cts", "cpr")
    ag_c(0)
    ag_a(1)
    ag_b(1)
    loads["cc2"].wait()
    turned(w2.at[0], w2t.at[0])
    ag_done(0)
    loads["cc1"].wait()
    conv_first(0, 0, 0)
    ag_c(1)
    conv_first(0, 0, 1)
    ag_a(2)
    ag_b(2)
    conv_first(0, 0, 2)
    second_operand(0, 1 - branch)
    conv_second(0, 0, 0)
    for h in range(PARTS):
        rs1(0, h)
    ag_c(2)
    conv_second(0, 0, 1)
    conv_second(0, 0, 2)
    for h in range(PARTS):
        rs2(0, h)
    conv_second(0, 0, 3)
    ag_done(1)
    conv_first(1, 0, 0)
    conv_first(1, 0, 1)
    for h in range(PARTS):
        rs3(0, h)
    conv_first(1, 0, 2)
    second_operand(0, branch)
    conv_second(1, 0, 0)
    for h in range(PARTS):
        rs1(1, h)
    conv_second(1, 0, 1)
    conv_second(1, 0, 2)
    for h in range(PARTS):
        rs2(1, h)
    conv_second(1, 0, 3)
    loads["zc"].wait()
    turned(zw, zt)
    scale = sc_ref[1 - branch, 0].astype(F32) * 0.125
    for h in range(PARTS):
        co[0:WIDTH, lanes(h)] = summed(0, h).astype(BF16)
    for c in range(4):
        for h in range(PARTS):
            zs[c, :, :, lanes(h)] = zero_terms(c, scale, h).astype(BF16)
    send(zs, zr, swap_send, swap_recv, partner)
    for h in range(PARTS):
        rs3(1, h)
    embed(1, "utf", "uts", "upr")
    loads["uc2"].wait()
    turned(w2.at[1], w2t.at[1])
    loads["uc1"].wait()
    ag_done(2)
    for dy in range(3):
        conv_first(2, 1, dy)
    second_operand(1, branch)
    for c in range(4):
        conv_second(2, 1, c)
    arrived(zr, swap_recv, swap_send)
    for c in range(4):
        part[2, c] += zr[c].astype(F32)
    scale = sc_ref[branch, 0].astype(F32) * 0.125
    for h in range(PARTS):
        co[0:WIDTH, lanes(h)] = summed(1, h).astype(BF16)
        part[2, 0, :, :, lanes(h)] += zero_terms(0, scale, h)
        rs1(2, h)
        for c in range(1, 4):
            part[2, c, :, :, lanes(h)] += zero_terms(c, scale, h)
    for h in range(PARTS):
        rs2(2, h)
    for h in range(PARTS):
        rs3(2, h)
    for h in range(PARTS):
        out_ref[:, lanes(h)] = summed(2, h).astype(BF16)
    for copy in sent:
        copy.wait_send()


def shards(
    unet_hidden, control_hidden, timesteps, control_scales,
    unet_time_first, unet_time_second, unet_proj, unet_conv_first, unet_conv_second,
    control_time_first, control_time_second, control_proj, control_conv_first, control_conv_second,
    zero_conv,
):
    smem = pl.BlockSpec(memory_space=pltpu.SMEM)
    hbm = pl.BlockSpec(memory_space=pl.ANY)
    dma = pltpu.SemaphoreType.DMA
    out = pl.pallas_call(
        kernel,
        out_shape=jax.ShapeDtypeStruct((WIDTH, PIX), BF16),
        in_specs=[smem, smem] + [hbm] * 13,
        out_specs=pl.BlockSpec(memory_space=pltpu.VMEM),
        scratch_shapes=[
            pltpu.VMEM((3, WIDTH, PIX), BF16),
            pltpu.VMEM((3, C, PIX), BF16),
            pltpu.VMEM((2, TAPS * WIDTH, C), BF16),
            pltpu.VMEM((2, KPAD, C), BF16),
            pltpu.VMEM((2, C, KPAD), BF16),
            pltpu.VMEM((2, TDIM, C), BF16),
            pltpu.VMEM((2, C, C), BF16),
            pltpu.VMEM((2, C, WIDTH), BF16),
            pltpu.VMEM((ZPAD, C), BF16),
            pltpu.VMEM((C, ZPAD), BF16),
            pltpu.VMEM((2, ZPAD, 128), F32),
            pltpu.VMEM((WIDTH, PIX), F32),
            pltpu.VMEM((KPAD, PIX), BF16),
            pltpu.VMEM((3, 4, 2, WIDTH, PIX), F32),
            pltpu.VMEM((ZPAD, PIX), BF16),
            pltpu.VMEM((4, 2, WIDTH, PIX), BF16),
            pltpu.VMEM((4, 2, WIDTH, PIX), BF16),
            pltpu.VMEM((3, PARTS, 2, WIDTH, LANES), BF16),
            pltpu.VMEM((3, PARTS, 2, 2, WIDTH, LANES), BF16),
            pltpu.VMEM((3, PARTS, WIDTH, LANES), BF16),
            pltpu.VMEM((3, PARTS, 2, 2, HALF, LANES), BF16),
            pltpu.VMEM((3, PARTS, 2, 2, WIDTH, LANES), BF16),
            pltpu.VMEM((3, PARTS, WIDTH, LANES), BF16),
            dma((14,)),
            dma((3, 9)),
            dma((3, 9)),
            dma((3, PARTS, 2)),
            dma((3, PARTS, 2)),
            dma((3, PARTS)),
            dma((3, PARTS, 2)),
            dma((3, PARTS, 2)),
            dma((3, PARTS)),
            dma,
            dma,
        ],
        compiler_params=pltpu.CompilerParams(
            collective_id=0, has_side_effects=True, vmem_limit_bytes=67043328
        ),
    )(
        timesteps,
        control_scales[0],
        unet_hidden[0],
        control_hidden[0].reshape(2, WIDTH, PIX),
        unet_time_first,
        unet_time_second,
        unet_proj,
        unet_conv_first.reshape(TAPS * WIDTH, C),
        unet_conv_second.reshape(TAPS * WIDTH, C),
        control_time_first[0],
        control_time_second[0],
        control_proj[0],
        control_conv_first[0].reshape(TAPS * WIDTH, C),
        control_conv_second[0].reshape(TAPS * WIDTH, C),
        zero_conv[0],
    )
    return out[None]


def solution(mesh):
    in_specs = (
        P(("branch", "dp"), "mp", None),
        P("branch", None, "dp", "mp", None),
        P(None, "dp"),
        P("branch", None, "dp"),
        P(),
        P(),
        P(None, "mp"),
        P(None, "mp", None),
        P(None, "mp", None),
        P("branch", None, None),
        P("branch", None, None),
        P("branch", None, "mp"),
        P("branch", None, "mp", None),
        P("branch", None, "mp", None),
        P("branch", "mp", None),
    )
    out_specs = P(("branch", "dp"), "mp", None)
    return jax.shard_map(shards, mesh=mesh, in_specs=in_specs, out_specs=out_specs, check_vma=False)
```

```python
import functools
import math

import jax
import jax.numpy as jnp
from jax import lax
from jax.experimental import pallas as pl
from jax.experimental.pallas import tpu as pltpu
from jax.sharding import PartitionSpec as P

C = 1280
TDIM = 320
SIDE = 16
PIX = 256
WIDTH = 160
GROUP = 40
HALF = 80
TAPS = 9
KPAD = 1536
ZPAD = 256
PARTS = 2
LANES = PIX // PARTS
MESH = pl.DeviceIdType.MESH
F32 = jnp.float32
BF16 = jnp.bfloat16


def silu(v):
    return v * 0.5 * (1.0 + jnp.tanh(v * 0.5))


def norm_silu(values):
    grouped = values.reshape(WIDTH // GROUP, GROUP, PIX)
    scale = 1.0 / (GROUP * PIX)
    mean = jnp.sum(jnp.sum(grouped, axis=1, keepdims=True), axis=2, keepdims=True) * scale
    centered = grouped - mean
    var = jnp.sum(jnp.sum(centered * centered, axis=1, keepdims=True), axis=2, keepdims=True) * scale
    return silu(centered * lax.rsqrt(var + 1e-05)).reshape(WIDTH, PIX)


def shifted(values, step, pixel):
    return pltpu.roll(values, (-step) % PIX, 1)


def kernel(
    ts_ref, sc_ref, uh, ch, utf, uts, upr, uc1, uc2, ctf, cts, cpr, cc1, cc2, zc,
    out_ref,
    hid, act, w1, w2, w2t, tf, tw, pr, zw, zt, tpt, inner, shifts, part, co, zs, zr,
    st1, st2, st3, r1, r2, r3,
    load_sem, ag_send, ag_recv, s1, s2, s3, v1, v2, v3, swap_send, swap_recv,
):
    branch = lax.axis_index("branch")
    spot = lax.axis_index("mp")
    z = spot // 4
    y = spot % 4
    zo = 1 - z
    yp, ym, y2 = (y + 1) % 4, (y + 3) % 4, (y + 2) % 4
    up = {"mp": z * 4 + yp}
    down = {"mp": z * 4 + ym}
    across = {"mp": zo * 4 + y}
    across_up = {"mp": zo * 4 + yp}
    across_down = {"mp": zo * 4 + ym}
    partner = {"branch": 1 - branch}
    columns = (y2, yp, ym, y)

    sent = []

    def send(src, dst, ssem, rsem, target):
        copy = pltpu.make_async_remote_copy(
            src_ref=src, dst_ref=dst, send_sem=ssem, recv_sem=rsem, device_id=target, device_id_type=MESH
        )
        copy.start()
        sent.append(copy)

    def arrived(dst, rsem, ssem):
        pltpu.make_async_remote_copy(
            src_ref=dst, dst_ref=dst, send_sem=ssem, recv_sem=rsem, device_id=up, device_id_type=MESH
        ).wait_recv()

    barrier = pltpu.get_barrier_semaphore()
    for target in (up, down, across, partner):
        pl.semaphore_signal(barrier, inc=1, device_id=target, device_id_type=MESH)

    loads = {}

    def load(name, src, dst):
        loads[name] = pltpu.make_async_copy(src, dst, load_sem.at[len(loads)])
        loads[name].start()

    load("h0", ch.at[1 - branch], hid.at[0])
    load("h1", ch.at[branch], hid.at[1])
    load("h2", uh, hid.at[2])
    load("ctf", ctf, tf.at[0])
    load("cts", cts, tw.at[0])
    load("cpr", cpr, pr.at[0])
    load("cc1", cc1, w1.at[0])
    load("cc2", cc2, w2.at[0, pl.ds(0, TAPS * WIDTH)])
    load("utf", utf, tf.at[1])
    load("uts", uts, tw.at[1])
    load("upr", upr, pr.at[1])
    load("zc", zc, zw.at[pl.ds(0, WIDTH)])
    load("uc1", uc1, w1.at[1])
    load("uc2", uc2, w2.at[1, pl.ds(0, TAPS * WIDTH)])

    def rows(zz, yy):
        return pl.multiple_of((zz * 4 + yy) * WIDTH, 32)

    def piece(i, zz, yy, start=0, size=WIDTH):
        return act.at[i, pl.ds(pl.multiple_of(rows(zz, yy) + start, 16), size)]

    def normed(i, name):
        loads[name].wait()
        act[i, pl.ds(rows(z, y), WIDTH), :] = norm_silu(hid[i].astype(F32)).astype(BF16)

    def ag_own(i):
        own = piece(i, z, y)
        send(own, own, ag_send.at[i, 0], ag_recv.at[i, 0], across)
        send(own, own, ag_send.at[i, 1], ag_recv.at[i, 1], up)
        send(own, own, ag_send.at[i, 2], ag_recv.at[i, 2], down)

    def ag_a(i):
        got = piece(i, zo, y)
        arrived(got, ag_recv.at[i, 0], ag_send.at[i, 0])
        send(got, got, ag_send.at[i, 3], ag_recv.at[i, 3], up)
        send(got, got, ag_send.at[i, 4], ag_recv.at[i, 4], down)

    def ag_b(i):
        arrived(piece(i, z, ym), ag_recv.at[i, 1], ag_send.at[i, 1])
        low = piece(i, z, ym, 0, HALF)
        send(low, low, ag_send.at[i, 5], ag_recv.at[i, 5], up)
        arrived(piece(i, z, yp), ag_recv.at[i, 2], ag_send.at[i, 2])
        high = piece(i, z, yp, HALF, HALF)
        send(high, high, ag_send.at[i, 6], ag_recv.at[i, 6], down)

    def ag_c(i):
        for k in range(2):
            got = piece(i, z, y2, k * HALF, HALF)
            arrived(got, ag_recv.at[i, 5 + k], ag_send.at[i, 5 + k])
            send(got, got, ag_send.at[i, 7 + k], ag_recv.at[i, 7 + k], across)

    def ag_done(i):
        arrived(piece(i, zo, ym), ag_recv.at[i, 3], ag_send.at[i, 3])
        arrived(piece(i, zo, yp), ag_recv.at[i, 4], ag_send.at[i, 4])
        for k in range(2):
            arrived(piece(i, zo, y2, k * HALF, HALF), ag_recv.at[i, 7 + k], ag_send.at[i, 7 + k])

    pixel = lax.broadcasted_iota(jnp.int32, (1, PIX), 1)
    column = pixel % SIDE
    not_left, not_right = column >= 1, column <= SIDE - 2
    not_top, not_bottom = pixel >= SIDE, pixel < PIX - SIDE

    def waves():
        lane = lax.broadcasted_iota(jnp.int32, (16, TDIM), 1)
        row = lax.broadcasted_iota(jnp.int32, (16, TDIM), 0)
        half_width = TDIM // 2
        index = jnp.where(lane < half_width, lane, lane - half_width).astype(F32)
        frequency = jnp.exp(-math.log(10000.0) * index / half_width)
        step = jnp.where(row == 0, ts_ref[0, 0].astype(F32), ts_ref[0, 1].astype(F32))
        angle = step * frequency
        return jnp.where(lane < half_width, jnp.cos(angle), jnp.sin(angle)).astype(BF16)

    def embed(k, first, second, third):
        loads[first].wait()
        middle = silu(jnp.dot(waves(), tf[k], preferred_element_type=F32)).astype(BF16)
        loads[second].wait()
        time_act = silu(jnp.dot(middle, tw[k], preferred_element_type=F32)).astype(BF16)
        loads[third].wait()
        tpt[k] = lax.dot_general(pr[k], time_act, (((1,), (1,)), ((), ())), preferred_element_type=F32)

    def time_column(k, half):
        lane = lax.broadcasted_iota(jnp.int32, (WIDTH, 16), 1)
        return jnp.sum(jnp.where(lane == half, tpt[k], 0.0), axis=1, keepdims=True)

    def turned(src, dst):
        def body(j, carry):
            at = pl.multiple_of(j * 128, 128)
            dst[pl.ds(at, 128), :] = src[:, pl.ds(at, 128)].T
            return carry

        lax.fori_loop(0, C // 128, body, 0)

    def conv_first(i, k, dy):
        product = jnp.dot(
            w1[k, dy * 3 * WIDTH : (dy + 1) * 3 * WIDTH, :], act[i], preferred_element_type=F32
        )
        left = jnp.where(not_left, shifted(product[0:WIDTH], -1, pixel), 0.0)
        right = jnp.where(not_right, shifted(product[2 * WIDTH : 3 * WIDTH], 1, pixel), 0.0)
        total = left + product[WIDTH : 2 * WIDTH] + right
        if dy == 0:
            inner[...] = jnp.where(not_top, shifted(total, -SIDE, pixel), 0.0)
        elif dy == 1:
            inner[...] += total
        else:
            inner[...] += jnp.where(not_bottom, shifted(total, SIDE, pixel), 0.0)

    def second_operand(k, half):
        second = norm_silu(inner[...] + time_column(k, half))
        left = jnp.where(not_left, shifted(second, -1, pixel), 0.0)
        right = jnp.where(not_right, shifted(second, 1, pixel), 0.0)
        for dx, value in enumerate((left, second, right)):
            top = jnp.where(not_top, shifted(value, -SIDE, pixel), 0.0)
            bottom = jnp.where(not_bottom, shifted(value, SIDE, pixel), 0.0)
            for dy, moved in enumerate((top, value, bottom)):
                at = (dy * 3 + dx) * WIDTH
                shifts[at : at + WIDTH, :] = moved.astype(BF16)

    def both_planes(ref, yy):
        return jnp.concatenate([ref[pl.ds(rows(0, yy), WIDTH), :], ref[pl.ds(rows(1, yy), WIDTH), :]], axis=0)

    def conv_second(i, k, c):
        product = jnp.dot(both_planes(w2t.at[k], columns[c]), shifts[...], preferred_element_type=F32)
        part[i, c] = product.reshape(2, WIDTH, PIX)

    def lanes(h):
        return slice(h * LANES, (h + 1) * LANES)

    def rs1(i, h):
        st1[i, h] = part[i, 0, :, :, lanes(h)].astype(BF16)
        send(st1.at[i, h, :, pl.ds(0, HALF)], r1.at[i, h, 0], s1.at[i, h, 0], v1.at[i, h, 0], up)
        send(st1.at[i, h, :, pl.ds(HALF, HALF)], r1.at[i, h, 1], s1.at[i, h, 1], v1.at[i, h, 1], down)

    def rsz(i, h):
        st3[i, h] = part[i, 3, zo, :, lanes(h)].astype(BF16)
        send(st3.at[i, h], r3.at[i, h], s3.at[i, h], v3.at[i, h], across)

    def rs2(i, h):
        for side, near, far in ((0, up, across_up), (1, down, across_down)):
            arrived(r1.at[i, h, side], v1.at[i, h, side], s1.at[i, h, side])
            plus = slice(side * HALF, (side + 1) * HALF)
            other = slice((1 - side) * HALF, (2 - side) * HALF)
            st2[i, h, side, :, plus, :] = (
                part[i, 1 + side, :, plus, lanes(h)] + r1[i, h, side].astype(F32)
            ).astype(BF16)
            st2[i, h, side, :, other, :] = part[i, 1 + side, :, other, lanes(h)].astype(BF16)
            for plane, zz, target in ((1, zo, far), (0, z, near)):
                send(
                    st2.at[i, h, side, zz], r2.at[i, h, side, plane],
                    s2.at[i, h, side, plane], v2.at[i, h, side, plane], target,
                )

    def summed(i, h):
        total = hid[i, :, lanes(h)].astype(F32) + part[i, 3, z, :, lanes(h)]
        arrived(r3.at[i, h], v3.at[i, h], s3.at[i, h])
        total = total + r3[i, h].astype(F32)
        for plane in range(2):
            for side in range(2):
                arrived(r2.at[i, h, side, plane], v2.at[i, h, side, plane], s2.at[i, h, side, plane])
                total = total + r2[i, h, side, plane].astype(F32)
        return total

    def zero_terms(c, scale, h):
        product = jnp.dot(both_planes(zt, columns[c]), co[:, lanes(h)], preferred_element_type=F32)
        return (product * scale).reshape(2, WIDTH, LANES)

    normed(0, "h0")
    pl.semaphore_wait(barrier, 4)
    ag_own(0)
    normed(1, "h1")
    ag_own(1)
    normed(2, "h2")
    for k in range(2):
        w2[k, TAPS * WIDTH : KPAD, :] = jnp.zeros((KPAD - TAPS * WIDTH, C), BF16)
    shifts[TAPS * WIDTH : KPAD, :] = jnp.zeros((KPAD - TAPS * WIDTH, PIX), BF16)
    zw[WIDTH:ZPAD, :] = jnp.zeros((ZPAD - WIDTH, C), BF16)
    co[WIDTH:ZPAD, :] = jnp.zeros((ZPAD - WIDTH, PIX), BF16)
    ag_a(0)
    ag_b(0)
    embed(0, "ctf", "cts", "cpr")
    ag_c(0)
    ag_a(1)
    ag_b(1)
    ag_own(2)
    loads["cc2"].wait()
    turned(w2.at[0], w2t.at[0])
    loads["cc1"].wait()
    ag_c(1)
    ag_done(0)
    conv_first(0, 0, 0)
    conv_first(0, 0, 1)
    ag_a(2)
    conv_first(0, 0, 2)
    ag_b(2)
    second_operand(0, 1 - branch)
    conv_second(0, 0, 0)
    for h in range(PARTS):
        rs1(0, h)
    conv_second(0, 0, 3)
    for h in range(PARTS):
        rsz(0, h)
    conv_second(0, 0, 1)
    conv_second(0, 0, 2)
    ag_c(2)
    ag_done(1)
    conv_first(1, 0, 0)
    for h in range(PARTS):
        rs2(0, h)
    conv_first(1, 0, 1)
    conv_first(1, 0, 2)
    second_operand(0, branch)
    conv_second(1, 0, 0)
    for h in range(PARTS):
        rs1(1, h)
    conv_second(1, 0, 3)
    for h in range(PARTS):
        rsz(1, h)
    conv_second(1, 0, 1)
    conv_second(1, 0, 2)
    loads["zc"].wait()
    turned(zw, zt)
    for h in range(PARTS):
        rs2(1, h)
    scale = sc_ref[0, 1 - branch].astype(F32) * 0.125
    for h in range(PARTS):
        co[0:WIDTH, lanes(h)] = summed(0, h).astype(BF16)
    for c in range(4):
        for h in range(PARTS):
            zs[c, :, :, lanes(h)] = zero_terms(c, scale, h).astype(BF16)
    send(zs, zr, swap_send, swap_recv, partner)
    embed(1, "utf", "uts", "upr")
    loads["uc2"].wait()
    turned(w2.at[1], w2t.at[1])
    loads["uc1"].wait()
    ag_done(2)
    for dy in range(3):
        conv_first(2, 1, dy)
    second_operand(1, branch)
    for c in range(4):
        conv_second(2, 1, c)
    arrived(zr, swap_recv, swap_send)
    for c in range(4):
        part[2, c] += zr[c].astype(F32)
    scale = sc_ref[0, branch].astype(F32) * 0.125
    for h in range(PARTS):
        co[0:WIDTH, lanes(h)] = summed(1, h).astype(BF16)
        part[2, 0, :, :, lanes(h)] += zero_terms(0, scale, h)
        rs1(2, h)
        part[2, 3, :, :, lanes(h)] += zero_terms(3, scale, h)
        rsz(2, h)
        for c in range(1, 3):
            part[2, c, :, :, lanes(h)] += zero_terms(c, scale, h)
    for h in range(PARTS):
        rs2(2, h)
    for h in range(PARTS):
        out_ref[:, lanes(h)] = summed(2, h).astype(BF16)
    for copy in sent:
        copy.wait_send()


def shards(
    unet_hidden, control_hidden, timesteps, control_scales,
    unet_time_first, unet_time_second, unet_proj, unet_conv_first, unet_conv_second,
    control_time_first, control_time_second, control_proj, control_conv_first, control_conv_second,
    zero_conv,
):
    smem = pl.BlockSpec(memory_space=pltpu.SMEM)
    hbm = pl.BlockSpec(memory_space=pl.ANY)
    dma = pltpu.SemaphoreType.DMA
    out = pl.pallas_call(
        kernel,
        out_shape=jax.ShapeDtypeStruct((WIDTH, PIX), BF16),
        in_specs=[smem, smem] + [hbm] * 13,
        out_specs=pl.BlockSpec(memory_space=pltpu.VMEM),
        scratch_shapes=[
            pltpu.VMEM((3, WIDTH, PIX), BF16),
            pltpu.VMEM((3, C, PIX), BF16),
            pltpu.VMEM((2, TAPS * WIDTH, C), BF16),
            pltpu.VMEM((2, KPAD, C), BF16),
            pltpu.VMEM((2, C, KPAD), BF16),
            pltpu.VMEM((2, TDIM, C), BF16),
            pltpu.VMEM((2, C, C), BF16),
            pltpu.VMEM((2, WIDTH, C), BF16),
            pltpu.VMEM((ZPAD, C), BF16),
            pltpu.VMEM((C, ZPAD), BF16),
            pltpu.VMEM((2, WIDTH, 16), F32),
            pltpu.VMEM((WIDTH, PIX), F32),
            pltpu.VMEM((KPAD, PIX), BF16),
            pltpu.VMEM((3, 4, 2, WIDTH, PIX), F32),
            pltpu.VMEM((ZPAD, PIX), BF16),
            pltpu.VMEM((4, 2, WIDTH, PIX), BF16),
            pltpu.VMEM((4, 2, WIDTH, PIX), BF16),
            pltpu.VMEM((3, PARTS, 2, WIDTH, LANES), BF16),
            pltpu.VMEM((3, PARTS, 2, 2, WIDTH, LANES), BF16),
            pltpu.VMEM((3, PARTS, WIDTH, LANES), BF16),
            pltpu.VMEM((3, PARTS, 2, 2, HALF, LANES), BF16),
            pltpu.VMEM((3, PARTS, 2, 2, WIDTH, LANES), BF16),
            pltpu.VMEM((3, PARTS, WIDTH, LANES), BF16),
            dma((14,)),
            dma((3, 9)),
            dma((3, 9)),
            dma((3, PARTS, 2)),
            dma((3, PARTS, 2, 2)),
            dma((3, PARTS)),
            dma((3, PARTS, 2)),
            dma((3, PARTS, 2, 2)),
            dma((3, PARTS)),
            dma,
            dma,
        ],
        compiler_params=pltpu.CompilerParams(
            collective_id=0, has_side_effects=True, vmem_limit_bytes=67043328
        ),
    )(
        timesteps.reshape(1, 2),
        control_scales.reshape(1, 2),
        unet_hidden[0],
        control_hidden[0].reshape(2, WIDTH, PIX),
        unet_time_first,
        unet_time_second,
        unet_proj.T,
        unet_conv_first.reshape(TAPS * WIDTH, C),
        unet_conv_second.reshape(TAPS * WIDTH, C),
        control_time_first[0],
        control_time_second[0],
        control_proj[0].T,
        control_conv_first[0].reshape(TAPS * WIDTH, C),
        control_conv_second[0].reshape(TAPS * WIDTH, C),
        zero_conv[0],
    )
    return out[None]


def solution(mesh):
    in_specs = (
        P(("branch", "dp"), "mp", None),
        P("branch", None, "dp", "mp", None),
        P(None, "dp"),
        P("branch", None, "dp"),
        P(),
        P(),
        P(None, "mp"),
        P(None, "mp", None),
        P(None, "mp", None),
        P("branch", None, None),
        P("branch", None, None),
        P("branch", None, "mp"),
        P("branch", None, "mp", None),
        P("branch", None, "mp", None),
        P("branch", "mp", None),
    )
    out_specs = P(("branch", "dp"), "mp", None)
    return jax.shard_map(shards, mesh=mesh, in_specs=in_specs, out_specs=out_specs, check_vma=False)
```

```python
import functools
import math

import jax
import jax.numpy as jnp
from jax import lax
from jax.experimental import pallas as pl
from jax.experimental.pallas import tpu as pltpu
from jax.sharding import PartitionSpec as P

C = 1280
TDIM = 320
SIDE = 16
PIX = 256
WIDTH = 160
GROUP = 40
HALF = 80
TAPS = 9
KPAD = 1536
ZPAD = 256
PARTS = 2
LANES = PIX // PARTS
MESH = pl.DeviceIdType.MESH
F32 = jnp.float32
BF16 = jnp.bfloat16


def silu(v):
    return v * 0.5 * (1.0 + jnp.tanh(v * 0.5))


def norm_silu(values):
    grouped = values.reshape(WIDTH // GROUP, GROUP, PIX)
    scale = 1.0 / (GROUP * PIX)
    mean = jnp.sum(jnp.sum(grouped, axis=1, keepdims=True), axis=2, keepdims=True) * scale
    centered = grouped - mean
    var = jnp.sum(jnp.sum(centered * centered, axis=1, keepdims=True), axis=2, keepdims=True) * scale
    return silu(centered * lax.rsqrt(var + 1e-05)).reshape(WIDTH, PIX)


def shifted(values, step, pixel):
    return pltpu.roll(values, (-step) % PIX, 1)


def kernel(
    ts_ref, sc_ref, uh, ch, utf, uts, upr, uc1, uc2, ctf, cts, cpr, cc1, cc2, zc,
    out_ref,
    hid, act, w1, w2, w2t, tf, tw, pr, zw, zt, tpt, inner, shifts, part, co, zs, zr,
    st1, st2, st3, r1, r2, r3,
    gate, load_sem, ag_send, ag_recv, s1, s2, s3, v1, v2, v3, swap_send, swap_recv,
):
    branch = lax.axis_index("branch")
    spot = lax.axis_index("mp")
    z = spot // 4
    y = spot % 4
    zo = 1 - z
    yp, ym, y2 = (y + 1) % 4, (y + 3) % 4, (y + 2) % 4
    up = {"mp": z * 4 + yp}
    down = {"mp": z * 4 + ym}
    across = {"mp": zo * 4 + y}
    across_up = {"mp": zo * 4 + yp}
    across_down = {"mp": zo * 4 + ym}
    partner = {"branch": 1 - branch}
    columns = (y2, yp, ym, y)

    sent = []

    def send(src, dst, ssem, rsem, target):
        copy = pltpu.make_async_remote_copy(
            src_ref=src, dst_ref=dst, send_sem=ssem, recv_sem=rsem, device_id=target, device_id_type=MESH
        )
        copy.start()
        sent.append(copy)

    def arrived(dst, rsem, ssem):
        pltpu.make_async_remote_copy(
            src_ref=dst, dst_ref=dst, send_sem=ssem, recv_sem=rsem, device_id=up, device_id_type=MESH
        ).wait_recv()

    barrier = pltpu.get_barrier_semaphore()
    for target in (up, down, across, partner):
        pl.semaphore_signal(barrier, inc=1, device_id=target, device_id_type=MESH)

    loads = {}

    def load(name, src, dst):
        loads[name] = pltpu.make_async_copy(src, dst, load_sem.at[len(loads)])
        loads[name].start()

    load("h0", ch.at[1 - branch], hid.at[0])
    load("h1", ch.at[branch], hid.at[1])
    load("h2", uh, hid.at[2])
    load("ctf", ctf, tf.at[0])
    load("cts", cts, tw.at[0])
    load("cpr", cpr, pr.at[0])
    load("cc1", cc1, w1.at[0])
    load("cc2", cc2, w2.at[0, pl.ds(0, TAPS * WIDTH)])
    load("utf", utf, tf.at[1])
    load("uts", uts, tw.at[1])
    load("upr", upr, pr.at[1])
    load("zc", zc, zw.at[pl.ds(0, WIDTH)])
    load("uc1", uc1, w1.at[1])
    load("uc2", uc2, w2.at[1, pl.ds(0, TAPS * WIDTH)])

    def rows(zz, yy):
        return pl.multiple_of((zz * 4 + yy) * WIDTH, 32)

    def piece(i, zz, yy, start=0, size=WIDTH):
        return act.at[i, pl.ds(pl.multiple_of(rows(zz, yy) + start, 16), size)]

    def normed(i, name):
        loads[name].wait()
        act[i, pl.ds(rows(z, y), WIDTH), :] = norm_silu(hid[i].astype(F32)).astype(BF16)

    def ag_near(i):
        own = piece(i, z, y)
        for k, target in ((1, up), (2, down), (0, across)):
            send(own, own, ag_send.at[i, k], ag_recv.at[i, k], target)

    def ag_far(i):
        own = piece(i, z, y)
        for k, target in ((3, across_up), (4, across_down)):
            send(own, own, ag_send.at[i, k], ag_recv.at[i, k], target)

    def ag_relay(i, k):
        zz = z if k < 3 else zo
        side = (k - 1) % 2
        source, target = ((ym, up), (yp, down))[side]
        arrived(piece(i, zz, source), ag_recv.at[i, k], ag_send.at[i, k])
        half = piece(i, zz, source, side * HALF, HALF)
        send(half, half, ag_send.at[i, k + 4], ag_recv.at[i, k + 4], target)

    def ag_done(i):
        arrived(piece(i, zo, y), ag_recv.at[i, 0], ag_send.at[i, 0])
        for zz, first in ((z, 5), (zo, 7)):
            for k in range(2):
                arrived(piece(i, zz, y2, k * HALF, HALF), ag_recv.at[i, first + k], ag_send.at[i, first + k])

    pixel = lax.broadcasted_iota(jnp.int32, (1, PIX), 1)
    column = pixel % SIDE
    not_left, not_right = column >= 1, column <= SIDE - 2
    not_top, not_bottom = pixel >= SIDE, pixel < PIX - SIDE

    def waves():
        lane = lax.broadcasted_iota(jnp.int32, (16, TDIM), 1)
        row = lax.broadcasted_iota(jnp.int32, (16, TDIM), 0)
        half_width = TDIM // 2
        index = jnp.where(lane < half_width, lane, lane - half_width).astype(F32)
        frequency = jnp.exp(-math.log(10000.0) * index / half_width)
        step = jnp.where(row == 0, ts_ref[0, 0].astype(F32), ts_ref[0, 1].astype(F32))
        angle = step * frequency
        return jnp.where(lane < half_width, jnp.cos(angle), jnp.sin(angle)).astype(BF16)

    def embed(k, first, second, third):
        loads[first].wait()
        middle = silu(jnp.dot(waves(), tf[k], preferred_element_type=F32)).astype(BF16)
        loads[second].wait()
        time_act = silu(jnp.dot(middle, tw[k], preferred_element_type=F32)).astype(BF16)
        loads[third].wait()
        tpt[k] = lax.dot_general(pr[k], time_act, (((1,), (1,)), ((), ())), preferred_element_type=F32)

    def time_column(k, half):
        lane = lax.broadcasted_iota(jnp.int32, (WIDTH, 16), 1)
        return jnp.sum(jnp.where(lane == half, tpt[k], 0.0), axis=1, keepdims=True)

    def turned(src, dst):
        def body(j, carry):
            at = pl.multiple_of(j * 128, 128)
            dst[pl.ds(at, 128), :] = src[:, pl.ds(at, 128)].T
            return carry

        lax.fori_loop(0, C // 128, body, 0)

    def conv_first(i, k, dy):
        product = jnp.dot(
            w1[k, dy * 3 * WIDTH : (dy + 1) * 3 * WIDTH, :], act[i], preferred_element_type=F32
        )
        left = jnp.where(not_left, shifted(product[0:WIDTH], -1, pixel), 0.0)
        right = jnp.where(not_right, shifted(product[2 * WIDTH : 3 * WIDTH], 1, pixel), 0.0)
        total = left + product[WIDTH : 2 * WIDTH] + right
        if dy == 0:
            inner[...] = jnp.where(not_top, shifted(total, -SIDE, pixel), 0.0)
        elif dy == 1:
            inner[...] += total
        else:
            inner[...] += jnp.where(not_bottom, shifted(total, SIDE, pixel), 0.0)

    def second_operand(k, half):
        second = norm_silu(inner[...] + time_column(k, half))
        left = jnp.where(not_left, shifted(second, -1, pixel), 0.0)
        right = jnp.where(not_right, shifted(second, 1, pixel), 0.0)
        for dx, value in enumerate((left, second, right)):
            top = jnp.where(not_top, shifted(value, -SIDE, pixel), 0.0)
            bottom = jnp.where(not_bottom, shifted(value, SIDE, pixel), 0.0)
            for dy, moved in enumerate((top, value, bottom)):
                at = (dy * 3 + dx) * WIDTH
                shifts[at : at + WIDTH, :] = moved.astype(BF16)

    def both_planes(ref, yy):
        return jnp.concatenate([ref[pl.ds(rows(0, yy), WIDTH), :], ref[pl.ds(rows(1, yy), WIDTH), :]], axis=0)

    def conv_second(i, k, c):
        product = jnp.dot(both_planes(w2t.at[k], columns[c]), shifts[...], preferred_element_type=F32)
        part[i, c] = product.reshape(2, WIDTH, PIX)

    def lanes(h):
        return slice(h * LANES, (h + 1) * LANES)

    def rs1(i, h):
        st1[i, h] = part[i, 0, :, :, lanes(h)].astype(BF16)
        send(st1.at[i, h, :, pl.ds(0, HALF)], r1.at[i, h, 0], s1.at[i, h, 0], v1.at[i, h, 0], up)
        send(st1.at[i, h, :, pl.ds(HALF, HALF)], r1.at[i, h, 1], s1.at[i, h, 1], v1.at[i, h, 1], down)

    def rsz(i, h):
        st3[i, h] = part[i, 3, zo, :, lanes(h)].astype(BF16)
        send(st3.at[i, h], r3.at[i, h], s3.at[i, h], v3.at[i, h], across)

    def rs2(i, h, side):
        near, far = ((up, across_up), (down, across_down))[side]
        arrived(r1.at[i, h, side], v1.at[i, h, side], s1.at[i, h, side])
        plus = slice(side * HALF, (side + 1) * HALF)
        other = slice((1 - side) * HALF, (2 - side) * HALF)
        st2[i, h, side, :, plus, :] = (
            part[i, 1 + side, :, plus, lanes(h)] + r1[i, h, side].astype(F32)
        ).astype(BF16)
        st2[i, h, side, :, other, :] = part[i, 1 + side, :, other, lanes(h)].astype(BF16)
        for plane, zz, target in ((1, zo, far), (0, z, near)):
            send(
                st2.at[i, h, side, zz], r2.at[i, h, side, plane],
                s2.at[i, h, side, plane], v2.at[i, h, side, plane], target,
            )

    def summed(i, h):
        total = hid[i, :, lanes(h)].astype(F32) + part[i, 3, z, :, lanes(h)]
        arrived(r3.at[i, h], v3.at[i, h], s3.at[i, h])
        total = total + r3[i, h].astype(F32)
        for plane in range(2):
            for side in range(2):
                arrived(r2.at[i, h, side, plane], v2.at[i, h, side, plane], s2.at[i, h, side, plane])
                total = total + r2[i, h, side, plane].astype(F32)
        return total

    def zero_terms(i, c, h):
        scale = sc_ref[0, 1 - branch if i == 0 else branch].astype(F32) * 0.125
        product = jnp.dot(both_planes(zt, columns[c]), co[i, :, lanes(h)], preferred_element_type=F32)
        return (product * scale).reshape(2, WIDTH, LANES)

    def copy_out(i, h):
        co[i, 0:WIDTH, lanes(h)] = summed(i, h).astype(BF16)

    def swap(h):
        copy_out(0, h)
        for c in range(4):
            zs[h, c] = zero_terms(0, c, h).astype(BF16)
        send(zs.at[h], zr.at[h], swap_send.at[h], swap_recv.at[h], partner)

    def swapped(h):
        arrived(zr.at[h], swap_recv.at[h], swap_send.at[h])
        for c in range(4):
            part[2, c, :, :, lanes(h)] += zr[h, c].astype(F32)

    def with_zero(c, h):
        part[2, c, :, :, lanes(h)] += zero_terms(1, c, h)

    normed(0, "h0")
    pl.semaphore_wait(barrier, 4)
    ag_near(0)
    pl.semaphore_signal(gate, inc=1, device_id=across, device_id_type=MESH)
    normed(1, "h1")
    normed(2, "h2")
    pl.semaphore_wait(gate, 1)
    ag_far(0)
    ag_near(1)
    ag_far(1)
    for k in range(2):
        w2[k, TAPS * WIDTH : KPAD, :] = jnp.zeros((KPAD - TAPS * WIDTH, C), BF16)
        co[k, WIDTH:ZPAD, :] = jnp.zeros((ZPAD - WIDTH, PIX), BF16)
    shifts[TAPS * WIDTH : KPAD, :] = jnp.zeros((KPAD - TAPS * WIDTH, PIX), BF16)
    zw[WIDTH:ZPAD, :] = jnp.zeros((ZPAD - WIDTH, C), BF16)
    embed(0, "ctf", "cts", "cpr")
    ag_relay(0, 1)
    ag_relay(0, 2)
    ag_relay(0, 3)
    ag_relay(0, 4)
    loads["cc2"].wait()
    turned(w2.at[0], w2t.at[0])
    loads["cc1"].wait()
    ag_relay(1, 1)
    ag_relay(1, 2)
    ag_near(2)
    ag_far(2)
    ag_done(0)
    @pl.when(branch < 2)
    def _():
        conv_first(0, 0, 0)
        conv_first(0, 0, 1)
        conv_first(0, 0, 2)
    ag_relay(1, 3)
    ag_relay(1, 4)
    @pl.when(branch < 2)
    def _():
        second_operand(0, 1 - branch)
    @pl.when(branch < 2)
    def _():
        conv_second(0, 0, 0)
        conv_second(0, 0, 3)
    rs1(0, 0)
    rs1(0, 1)
    rsz(0, 0)
    rsz(0, 1)
    @pl.when(branch < 2)
    def _():
        conv_second(0, 0, 1)
        conv_second(0, 0, 2)
    ag_relay(2, 1)
    ag_relay(2, 2)
    ag_done(1)
    @pl.when(branch < 2)
    def _():
        conv_first(1, 0, 0)
        conv_first(1, 0, 1)
        conv_first(1, 0, 2)
    rs2(0, 0, 0)
    rs2(0, 0, 1)
    ag_relay(2, 3)
    ag_relay(2, 4)
    @pl.when(branch < 2)
    def _():
        second_operand(0, branch)
    @pl.when(branch < 2)
    def _():
        conv_second(1, 0, 0)
        conv_second(1, 0, 3)
    rs1(1, 0)
    rs1(1, 1)
    rsz(1, 0)
    rsz(1, 1)
    @pl.when(branch < 2)
    def _():
        conv_second(1, 0, 1)
        conv_second(1, 0, 2)
    rs2(0, 1, 0)
    rs2(0, 1, 1)
    loads["zc"].wait()
    turned(zw, zt)
    loads["uc2"].wait()
    turned(w2.at[1], w2t.at[1])
    embed(1, "utf", "uts", "upr")
    rs2(1, 0, 0)
    rs2(1, 0, 1)
    rs2(1, 1, 0)
    rs2(1, 1, 1)
    loads["uc1"].wait()
    ag_done(2)
    @pl.when(branch < 2)
    def _():
        conv_first(2, 1, 0)
        conv_first(2, 1, 1)
        conv_first(2, 1, 2)
    swap(0)
    swap(1)
    @pl.when(branch < 2)
    def _():
        second_operand(1, branch)
    @pl.when(branch < 2)
    def _():
        conv_second(2, 1, 0)
        conv_second(2, 1, 3)
        conv_second(2, 1, 1)
        conv_second(2, 1, 2)
    swapped(0)
    swapped(1)
    copy_out(1, 0)
    with_zero(0, 0)
    rs1(2, 0)
    with_zero(3, 0)
    rsz(2, 0)
    with_zero(1, 0)
    with_zero(2, 0)
    copy_out(1, 1)
    with_zero(0, 1)
    rs1(2, 1)
    with_zero(3, 1)
    rsz(2, 1)
    with_zero(1, 1)
    with_zero(2, 1)
    rs2(2, 0, 0)
    rs2(2, 0, 1)
    rs2(2, 1, 0)
    rs2(2, 1, 1)
    out_ref[:, lanes(0)] = summed(2, 0).astype(BF16)
    out_ref[:, lanes(1)] = summed(2, 1).astype(BF16)
    for copy in sent:
        copy.wait_send()


def shards(
    unet_hidden, control_hidden, timesteps, control_scales,
    unet_time_first, unet_time_second, unet_proj, unet_conv_first, unet_conv_second,
    control_time_first, control_time_second, control_proj, control_conv_first, control_conv_second,
    zero_conv,
):
    smem = pl.BlockSpec(memory_space=pltpu.SMEM)
    hbm = pl.BlockSpec(memory_space=pl.ANY)
    dma = pltpu.SemaphoreType.DMA
    out = pl.pallas_call(
        kernel,
        out_shape=jax.ShapeDtypeStruct((WIDTH, PIX), BF16),
        in_specs=[smem, smem] + [hbm] * 13,
        out_specs=pl.BlockSpec(memory_space=pltpu.VMEM),
        scratch_shapes=[
            pltpu.VMEM((3, WIDTH, PIX), BF16),
            pltpu.VMEM((3, C, PIX), BF16),
            pltpu.VMEM((2, TAPS * WIDTH, C), BF16),
            pltpu.VMEM((2, KPAD, C), BF16),
            pltpu.VMEM((2, C, KPAD), BF16),
            pltpu.VMEM((2, TDIM, C), BF16),
            pltpu.VMEM((2, C, C), BF16),
            pltpu.VMEM((2, WIDTH, C), BF16),
            pltpu.VMEM((ZPAD, C), BF16),
            pltpu.VMEM((C, ZPAD), BF16),
            pltpu.VMEM((2, WIDTH, 16), F32),
            pltpu.VMEM((WIDTH, PIX), F32),
            pltpu.VMEM((KPAD, PIX), BF16),
            pltpu.VMEM((3, 4, 2, WIDTH, PIX), F32),
            pltpu.VMEM((2, ZPAD, PIX), BF16),
            pltpu.VMEM((PARTS, 4, 2, WIDTH, LANES), BF16),
            pltpu.VMEM((PARTS, 4, 2, WIDTH, LANES), BF16),
            pltpu.VMEM((3, PARTS, 2, WIDTH, LANES), BF16),
            pltpu.VMEM((3, PARTS, 2, 2, WIDTH, LANES), BF16),
            pltpu.VMEM((3, PARTS, WIDTH, LANES), BF16),
            pltpu.VMEM((3, PARTS, 2, 2, HALF, LANES), BF16),
            pltpu.VMEM((3, PARTS, 2, 2, WIDTH, LANES), BF16),
            pltpu.VMEM((3, PARTS, WIDTH, LANES), BF16),
            pltpu.SemaphoreType.REGULAR,
            dma((14,)),
            dma((3, 9)),
            dma((3, 9)),
            dma((3, PARTS, 2)),
            dma((3, PARTS, 2, 2)),
            dma((3, PARTS)),
            dma((3, PARTS, 2)),
            dma((3, PARTS, 2, 2)),
            dma((3, PARTS)),
            dma((PARTS,)),
            dma((PARTS,)),
        ],
        compiler_params=pltpu.CompilerParams(
            collective_id=0, has_side_effects=True, vmem_limit_bytes=67043328
        ),
    )(
        timesteps.reshape(1, 2),
        control_scales.reshape(1, 2),
        unet_hidden[0],
        control_hidden[0].reshape(2, WIDTH, PIX),
        unet_time_first,
        unet_time_second,
        unet_proj.T,
        unet_conv_first.reshape(TAPS * WIDTH, C),
        unet_conv_second.reshape(TAPS * WIDTH, C),
        control_time_first[0],
        control_time_second[0],
        control_proj[0].T,
        control_conv_first[0].reshape(TAPS * WIDTH, C),
        control_conv_second[0].reshape(TAPS * WIDTH, C),
        zero_conv[0],
    )
    return out[None]


def solution(mesh):
    in_specs = (
        P(("branch", "dp"), "mp", None),
        P("branch", None, "dp", "mp", None),
        P(None, "dp"),
        P("branch", None, "dp"),
        P(),
        P(),
        P(None, "mp"),
        P(None, "mp", None),
        P(None, "mp", None),
        P("branch", None, None),
        P("branch", None, None),
        P("branch", None, "mp"),
        P("branch", None, "mp", None),
        P("branch", None, "mp", None),
        P("branch", "mp", None),
    )
    out_specs = P(("branch", "dp"), "mp", None)
    return jax.shard_map(shards, mesh=mesh, in_specs=in_specs, out_specs=out_specs, check_vma=False)
```

```python
import functools
import math

import jax
import jax.numpy as jnp
from jax import lax
from jax.experimental import pallas as pl
from jax.experimental.pallas import tpu as pltpu
from jax.sharding import PartitionSpec as P

C = 1280
TDIM = 320
SIDE = 16
PIX = 256
WIDTH = 160
GROUP = 40
HALF = 80
TAPS = 9
KPAD = 1536
ZPAD = 256
PARTS = 2
LANES = PIX // PARTS
MESH = pl.DeviceIdType.MESH
F32 = jnp.float32
BF16 = jnp.bfloat16


def silu(v):
    return v * 0.5 * (1.0 + jnp.tanh(v * 0.5))


def norm_silu(values):
    grouped = values.reshape(WIDTH // GROUP, GROUP, PIX)
    scale = 1.0 / (GROUP * PIX)
    mean = jnp.sum(jnp.sum(grouped, axis=1, keepdims=True), axis=2, keepdims=True) * scale
    centered = grouped - mean
    var = jnp.sum(jnp.sum(centered * centered, axis=1, keepdims=True), axis=2, keepdims=True) * scale
    return silu(centered * lax.rsqrt(var + 1e-05)).reshape(WIDTH, PIX)


def shifted(values, step, pixel):
    return pltpu.roll(values, (-step) % PIX, 1)


def kernel(
    ts_ref, sc_ref, uh, ch, utf, uts, upr, uc1, uc2, ctf, cts, cpr, cc1, cc2, zc,
    out_ref,
    hid, act, w1, w2, w2t, tf, tw, pr, zw, zt, tpt, inner, shifts, part, co, zs, zr,
    st1, st2, st3, r1, r2, r3,
    gate, load_sem, ag_send, ag_recv, s1, s2, s3, v1, v2, v3, swap_send, swap_recv,
):
    branch = lax.axis_index("branch")
    spot = lax.axis_index("mp")
    z = spot // 4
    y = spot % 4
    zo = 1 - z
    yp, ym, y2 = (y + 1) % 4, (y + 3) % 4, (y + 2) % 4
    up = {"mp": z * 4 + yp}
    down = {"mp": z * 4 + ym}
    across = {"mp": zo * 4 + y}
    across_up = {"mp": zo * 4 + yp}
    across_down = {"mp": zo * 4 + ym}
    partner = {"branch": 1 - branch}
    columns = (y2, yp, ym, y)

    sent = []

    def send(src, dst, ssem, rsem, target):
        copy = pltpu.make_async_remote_copy(
            src_ref=src, dst_ref=dst, send_sem=ssem, recv_sem=rsem, device_id=target, device_id_type=MESH
        )
        copy.start()
        sent.append(copy)

    def arrived(dst, rsem, ssem):
        pltpu.make_async_remote_copy(
            src_ref=dst, dst_ref=dst, send_sem=ssem, recv_sem=rsem, device_id=up, device_id_type=MESH
        ).wait_recv()

    barrier = pltpu.get_barrier_semaphore()
    for target in (up, down, across, partner):
        pl.semaphore_signal(barrier, inc=1, device_id=target, device_id_type=MESH)

    loads = {}

    def load(name, src, dst):
        loads[name] = pltpu.make_async_copy(src, dst, load_sem.at[len(loads)])
        loads[name].start()

    load("h0", ch.at[1 - branch], hid.at[0])
    load("h1", ch.at[branch], hid.at[1])
    load("h2", uh, hid.at[2])
    load("ctf", ctf, tf.at[0])
    load("cts", cts, tw.at[0])
    load("cpr", cpr, pr.at[0])
    load("cc1", cc1, w1.at[0])
    load("cc2", cc2, w2.at[0, pl.ds(0, TAPS * WIDTH)])
    load("utf", utf, tf.at[1])
    load("uts", uts, tw.at[1])
    load("upr", upr, pr.at[1])
    load("zc", zc, zw.at[pl.ds(0, WIDTH)])
    load("uc1", uc1, w1.at[1])
    load("uc2", uc2, w2.at[1, pl.ds(0, TAPS * WIDTH)])

    def rows(zz, yy):
        return pl.multiple_of((zz * 4 + yy) * WIDTH, 32)

    def piece(i, zz, yy, start=0, size=WIDTH):
        return act.at[i, pl.ds(pl.multiple_of(rows(zz, yy) + start, 16), size)]

    def normed(i, name):
        loads[name].wait()
        act[i, pl.ds(rows(z, y), WIDTH), :] = norm_silu(hid[i].astype(F32)).astype(BF16)

    def ag_near(i):
        own = piece(i, z, y)
        for k, target in ((1, up), (2, down), (0, across)):
            send(own, own, ag_send.at[i, k], ag_recv.at[i, k], target)

    def ag_far(i):
        own = piece(i, z, y)
        for k, target in ((3, across_up), (4, across_down)):
            send(own, own, ag_send.at[i, k], ag_recv.at[i, k], target)

    def ag_relay(i, k):
        zz = z if k < 3 else zo
        side = (k - 1) % 2
        source, target = ((ym, up), (yp, down))[side]
        arrived(piece(i, zz, source), ag_recv.at[i, k], ag_send.at[i, k])
        half = piece(i, zz, source, side * HALF, HALF)
        send(half, half, ag_send.at[i, k + 4], ag_recv.at[i, k + 4], target)

    def ag_cross(i):
        got = piece(i, zo, y)
        arrived(got, ag_recv.at[i, 0], ag_send.at[i, 0])
        for k, target in ((3, up), (4, down)):
            send(got, got, ag_send.at[i, k], ag_recv.at[i, k], target)

    def ag_over(i, k):
        got = piece(i, z, y2, k * HALF, HALF)
        arrived(got, ag_recv.at[i, 5 + k], ag_send.at[i, 5 + k])
        send(got, got, ag_send.at[i, 7 + k], ag_recv.at[i, 7 + k], across)

    def ag_done_over(i):
        arrived(piece(i, zo, ym), ag_recv.at[i, 3], ag_send.at[i, 3])
        arrived(piece(i, zo, yp), ag_recv.at[i, 4], ag_send.at[i, 4])
        for k in range(2):
            arrived(piece(i, zo, y2, k * HALF, HALF), ag_recv.at[i, 7 + k], ag_send.at[i, 7 + k])

    def ag_done(i):
        arrived(piece(i, zo, y), ag_recv.at[i, 0], ag_send.at[i, 0])
        for zz, first in ((z, 5), (zo, 7)):
            for k in range(2):
                arrived(piece(i, zz, y2, k * HALF, HALF), ag_recv.at[i, first + k], ag_send.at[i, first + k])

    pixel = lax.broadcasted_iota(jnp.int32, (1, PIX), 1)
    column = pixel % SIDE
    not_left, not_right = column >= 1, column <= SIDE - 2
    not_top, not_bottom = pixel >= SIDE, pixel < PIX - SIDE

    def waves():
        lane = lax.broadcasted_iota(jnp.int32, (16, TDIM), 1)
        row = lax.broadcasted_iota(jnp.int32, (16, TDIM), 0)
        half_width = TDIM // 2
        index = jnp.where(lane < half_width, lane, lane - half_width).astype(F32)
        frequency = jnp.exp(-math.log(10000.0) * index / half_width)
        step = jnp.where(row == 0, ts_ref[0, 0].astype(F32), ts_ref[0, 1].astype(F32))
        angle = step * frequency
        return jnp.where(lane < half_width, jnp.cos(angle), jnp.sin(angle)).astype(BF16)

    def embed(k, first, second, third):
        loads[first].wait()
        middle = silu(jnp.dot(waves(), tf[k], preferred_element_type=F32)).astype(BF16)
        loads[second].wait()
        time_act = silu(jnp.dot(middle, tw[k], preferred_element_type=F32)).astype(BF16)
        loads[third].wait()
        tpt[k] = lax.dot_general(pr[k], time_act, (((1,), (1,)), ((), ())), preferred_element_type=F32)

    def time_column(k, half):
        lane = lax.broadcasted_iota(jnp.int32, (WIDTH, 16), 1)
        return jnp.sum(jnp.where(lane == half, tpt[k], 0.0), axis=1, keepdims=True)

    def turned(src, dst):
        def body(j, carry):
            at = pl.multiple_of(j * 128, 128)
            dst[pl.ds(at, 128), :] = src[:, pl.ds(at, 128)].T
            return carry

        lax.fori_loop(0, C // 128, body, 0)

    def conv_first(i, k, dy):
        product = jnp.dot(
            w1[k, dy * 3 * WIDTH : (dy + 1) * 3 * WIDTH, :], act[i], preferred_element_type=F32
        )
        left = jnp.where(not_left, shifted(product[0:WIDTH], -1, pixel), 0.0)
        right = jnp.where(not_right, shifted(product[2 * WIDTH : 3 * WIDTH], 1, pixel), 0.0)
        total = left + product[WIDTH : 2 * WIDTH] + right
        if dy == 0:
            inner[...] = jnp.where(not_top, shifted(total, -SIDE, pixel), 0.0)
        elif dy == 1:
            inner[...] += total
        else:
            inner[...] += jnp.where(not_bottom, shifted(total, SIDE, pixel), 0.0)

    def second_operand(k, half):
        second = norm_silu(inner[...] + time_column(k, half))
        left = jnp.where(not_left, shifted(second, -1, pixel), 0.0)
        right = jnp.where(not_right, shifted(second, 1, pixel), 0.0)
        for dx, value in enumerate((left, second, right)):
            top = jnp.where(not_top, shifted(value, -SIDE, pixel), 0.0)
            bottom = jnp.where(not_bottom, shifted(value, SIDE, pixel), 0.0)
            for dy, moved in enumerate((top, value, bottom)):
                at = (dy * 3 + dx) * WIDTH
                shifts[at : at + WIDTH, :] = moved.astype(BF16)

    def both_planes(ref, yy):
        return jnp.concatenate([ref[pl.ds(rows(0, yy), WIDTH), :], ref[pl.ds(rows(1, yy), WIDTH), :]], axis=0)

    def conv_second(i, k, c):
        product = jnp.dot(both_planes(w2t.at[k], columns[c]), shifts[...], preferred_element_type=F32)
        part[i, c] = product.reshape(2, WIDTH, PIX)

    def lanes(h):
        return slice(h * LANES, (h + 1) * LANES)

    def rs1(i, h):
        st1[i, h] = part[i, 0, :, :, lanes(h)].astype(BF16)
        send(st1.at[i, h, :, pl.ds(0, HALF)], r1.at[i, h, 0], s1.at[i, h, 0], v1.at[i, h, 0], up)
        send(st1.at[i, h, :, pl.ds(HALF, HALF)], r1.at[i, h, 1], s1.at[i, h, 1], v1.at[i, h, 1], down)

    def rsz(i, h):
        st3[i, h] = part[i, 3, zo, :, lanes(h)].astype(BF16)
        send(st3.at[i, h], r3.at[i, h], s3.at[i, h], v3.at[i, h], across)

    def rs2(i, h, side):
        near, far = ((up, across_up), (down, across_down))[side]
        arrived(r1.at[i, h, side], v1.at[i, h, side], s1.at[i, h, side])
        plus = slice(side * HALF, (side + 1) * HALF)
        other = slice((1 - side) * HALF, (2 - side) * HALF)
        st2[i, h, side, :, plus, :] = (
            part[i, 1 + side, :, plus, lanes(h)] + r1[i, h, side].astype(F32)
        ).astype(BF16)
        st2[i, h, side, :, other, :] = part[i, 1 + side, :, other, lanes(h)].astype(BF16)
        for plane, zz, target in ((1, zo, far), (0, z, near)):
            send(
                st2.at[i, h, side, zz], r2.at[i, h, side, plane],
                s2.at[i, h, side, plane], v2.at[i, h, side, plane], target,
            )

    def summed(i, h):
        total = hid[i, :, lanes(h)].astype(F32) + part[i, 3, z, :, lanes(h)]
        arrived(r3.at[i, h], v3.at[i, h], s3.at[i, h])
        total = total + r3[i, h].astype(F32)
        for plane in range(2):
            for side in range(2):
                arrived(r2.at[i, h, side, plane], v2.at[i, h, side, plane], s2.at[i, h, side, plane])
                total = total + r2[i, h, side, plane].astype(F32)
        return total

    def zero_terms(i, c, h):
        scale = sc_ref[0, 1 - branch if i == 0 else branch].astype(F32) * 0.125
        product = jnp.dot(both_planes(zt, columns[c]), co[i, :, lanes(h)], preferred_element_type=F32)
        return (product * scale).reshape(2, WIDTH, LANES)

    def copy_out(i, h):
        co[i, 0:WIDTH, lanes(h)] = summed(i, h).astype(BF16)

    def swap(h):
        copy_out(0, h)
        for c in range(4):
            zs[h, c] = zero_terms(0, c, h).astype(BF16)
        send(zs.at[h], zr.at[h], swap_send.at[h], swap_recv.at[h], partner)

    def swapped(h):
        arrived(zr.at[h], swap_recv.at[h], swap_send.at[h])
        for c in range(4):
            part[2, c, :, :, lanes(h)] += zr[h, c].astype(F32)

    def with_zero(c, h):
        part[2, c, :, :, lanes(h)] += zero_terms(1, c, h)

    normed(0, "h0")
    pl.semaphore_wait(barrier, 4)
    ag_near(0)
    pl.semaphore_signal(gate, inc=1, device_id=across, device_id_type=MESH)
    normed(1, "h1")
    normed(2, "h2")
    pl.semaphore_wait(gate, 1)
    ag_far(0)
    ag_near(1)
    ag_far(1)
    for k in range(2):
        w2[k, TAPS * WIDTH : KPAD, :] = jnp.zeros((KPAD - TAPS * WIDTH, C), BF16)
        co[k, WIDTH:ZPAD, :] = jnp.zeros((ZPAD - WIDTH, PIX), BF16)
    shifts[TAPS * WIDTH : KPAD, :] = jnp.zeros((KPAD - TAPS * WIDTH, PIX), BF16)
    zw[WIDTH:ZPAD, :] = jnp.zeros((ZPAD - WIDTH, C), BF16)
    embed(0, "ctf", "cts", "cpr")
    ag_relay(0, 1)
    ag_relay(0, 2)
    ag_relay(0, 3)
    ag_relay(0, 4)
    loads["cc2"].wait()
    turned(w2.at[0], w2t.at[0])
    loads["cc1"].wait()
    ag_relay(1, 1)
    ag_relay(1, 2)
    ag_near(2)
    ag_far(2)
    ag_done(0)
    @pl.when(branch < 2)
    def _():
        conv_first(0, 0, 0)
        conv_first(0, 0, 1)
        conv_first(0, 0, 2)
    ag_relay(1, 3)
    ag_relay(1, 4)
    @pl.when(branch < 2)
    def _():
        second_operand(0, 1 - branch)
    @pl.when(branch < 2)
    def _():
        conv_second(0, 0, 0)
    rs1(0, 0)
    rs1(0, 1)
    @pl.when(branch < 2)
    def _():
        conv_second(0, 0, 3)
        conv_second(0, 0, 1)
        conv_second(0, 0, 2)
    rsz(0, 0)
    rsz(0, 1)
    ag_relay(2, 1)
    ag_relay(2, 2)
    ag_done(1)
    @pl.when(branch < 2)
    def _():
        conv_first(1, 0, 0)
        conv_first(1, 0, 1)
        conv_first(1, 0, 2)
    rs2(0, 0, 0)
    rs2(0, 0, 1)
    ag_relay(2, 3)
    ag_relay(2, 4)
    @pl.when(branch < 2)
    def _():
        second_operand(0, branch)
    @pl.when(branch < 2)
    def _():
        conv_second(1, 0, 0)
    rs1(1, 0)
    rs1(1, 1)
    @pl.when(branch < 2)
    def _():
        conv_second(1, 0, 3)
        conv_second(1, 0, 1)
        conv_second(1, 0, 2)
    rsz(1, 0)
    rsz(1, 1)
    rs2(0, 1, 0)
    rs2(0, 1, 1)
    loads["zc"].wait()
    turned(zw, zt)
    loads["uc2"].wait()
    turned(w2.at[1], w2t.at[1])
    embed(1, "utf", "uts", "upr")
    rs2(1, 0, 0)
    rs2(1, 0, 1)
    rs2(1, 1, 0)
    rs2(1, 1, 1)
    loads["uc1"].wait()
    ag_done(2)
    @pl.when(branch < 2)
    def _():
        conv_first(2, 1, 0)
        conv_first(2, 1, 1)
        conv_first(2, 1, 2)
    swap(0)
    swap(1)
    @pl.when(branch < 2)
    def _():
        second_operand(1, branch)
    @pl.when(branch < 2)
    def _():
        conv_second(2, 1, 0)
        conv_second(2, 1, 3)
        conv_second(2, 1, 1)
        conv_second(2, 1, 2)
    swapped(0)
    swapped(1)
    copy_out(1, 0)
    with_zero(0, 0)
    rs1(2, 0)
    with_zero(3, 0)
    rsz(2, 0)
    with_zero(1, 0)
    with_zero(2, 0)
    copy_out(1, 1)
    with_zero(0, 1)
    rs1(2, 1)
    with_zero(3, 1)
    rsz(2, 1)
    with_zero(1, 1)
    with_zero(2, 1)
    rs2(2, 0, 0)
    rs2(2, 0, 1)
    rs2(2, 1, 0)
    rs2(2, 1, 1)
    out_ref[:, lanes(0)] = summed(2, 0).astype(BF16)
    out_ref[:, lanes(1)] = summed(2, 1).astype(BF16)
    for copy in sent:
        copy.wait_send()


def shards(
    unet_hidden, control_hidden, timesteps, control_scales,
    unet_time_first, unet_time_second, unet_proj, unet_conv_first, unet_conv_second,
    control_time_first, control_time_second, control_proj, control_conv_first, control_conv_second,
    zero_conv,
):
    smem = pl.BlockSpec(memory_space=pltpu.SMEM)
    hbm = pl.BlockSpec(memory_space=pl.ANY)
    dma = pltpu.SemaphoreType.DMA
    out = pl.pallas_call(
        kernel,
        out_shape=jax.ShapeDtypeStruct((WIDTH, PIX), BF16),
        in_specs=[smem, smem] + [hbm] * 13,
        out_specs=pl.BlockSpec(memory_space=pltpu.VMEM),
        scratch_shapes=[
            pltpu.VMEM((3, WIDTH, PIX), BF16),
            pltpu.VMEM((3, C, PIX), BF16),
            pltpu.VMEM((2, TAPS * WIDTH, C), BF16),
            pltpu.VMEM((2, KPAD, C), BF16),
            pltpu.VMEM((2, C, KPAD), BF16),
            pltpu.VMEM((2, TDIM, C), BF16),
            pltpu.VMEM((2, C, C), BF16),
            pltpu.VMEM((2, WIDTH, C), BF16),
            pltpu.VMEM((ZPAD, C), BF16),
            pltpu.VMEM((C, ZPAD), BF16),
            pltpu.VMEM((2, WIDTH, 16), F32),
            pltpu.VMEM((WIDTH, PIX), F32),
            pltpu.VMEM((KPAD, PIX), BF16),
            pltpu.VMEM((3, 4, 2, WIDTH, PIX), F32),
            pltpu.VMEM((2, ZPAD, PIX), BF16),
            pltpu.VMEM((PARTS, 4, 2, WIDTH, LANES), BF16),
            pltpu.VMEM((PARTS, 4, 2, WIDTH, LANES), BF16),
            pltpu.VMEM((3, PARTS, 2, WIDTH, LANES), BF16),
            pltpu.VMEM((3, PARTS, 2, 2, WIDTH, LANES), BF16),
            pltpu.VMEM((3, PARTS, WIDTH, LANES), BF16),
            pltpu.VMEM((3, PARTS, 2, 2, HALF, LANES), BF16),
            pltpu.VMEM((3, PARTS, 2, 2, WIDTH, LANES), BF16),
            pltpu.VMEM((3, PARTS, WIDTH, LANES), BF16),
            pltpu.SemaphoreType.REGULAR,
            dma((14,)),
            dma((3, 9)),
            dma((3, 9)),
            dma((3, PARTS, 2)),
            dma((3, PARTS, 2, 2)),
            dma((3, PARTS)),
            dma((3, PARTS, 2)),
            dma((3, PARTS, 2, 2)),
            dma((3, PARTS)),
            dma((PARTS,)),
            dma((PARTS,)),
        ],
        compiler_params=pltpu.CompilerParams(
            collective_id=0, has_side_effects=True, vmem_limit_bytes=67043328
        ),
    )(
        timesteps.reshape(1, 2),
        control_scales.reshape(1, 2),
        unet_hidden[0],
        control_hidden[0].reshape(2, WIDTH, PIX),
        unet_time_first,
        unet_time_second,
        unet_proj.T,
        unet_conv_first.reshape(TAPS * WIDTH, C),
        unet_conv_second.reshape(TAPS * WIDTH, C),
        control_time_first[0],
        control_time_second[0],
        control_proj[0].T,
        control_conv_first[0].reshape(TAPS * WIDTH, C),
        control_conv_second[0].reshape(TAPS * WIDTH, C),
        zero_conv[0],
    )
    return out[None]


def solution(mesh):
    in_specs = (
        P(("branch", "dp"), "mp", None),
        P("branch", None, "dp", "mp", None),
        P(None, "dp"),
        P("branch", None, "dp"),
        P(),
        P(),
        P(None, "mp"),
        P(None, "mp", None),
        P(None, "mp", None),
        P("branch", None, None),
        P("branch", None, None),
        P("branch", None, "mp"),
        P("branch", None, "mp", None),
        P("branch", None, "mp", None),
        P("branch", "mp", None),
    )
    out_specs = P(("branch", "dp"), "mp", None)
    return jax.shard_map(shards, mesh=mesh, in_specs=in_specs, out_specs=out_specs, check_vma=False)
```
